256 devices in a mesh: groups: 2 (over y), seq: 32 (over z, core), role: 4 (over x).
Axes of the slice: x: 4, y: 2, z: 16, core: 2. Of those that a mesh axis runs over, the one named last changes fastest.
The devices are a block of a 4x16x16 slice.
Arguments:
- queries: bfloat16 [8, 4096, 4096], P(('groups', 'role'), 'seq'), parts along dimension 0, may hold values from -500 to 500
- keys: bfloat16 [8, 4096, 4096], P(('groups', 'role'), 'seq'), parts along dimension 0, may hold values from -500 to 500
- values: bfloat16 [8, 4096, 4096], P(('groups', 'role'), 'seq'), parts along dimension 0, may hold values from -6 to 6
- q_gain: float32 [4096], replicated, may hold values from 1.2 to 1.8
- k_gain: float32 [4096], replicated, may hold values from 1.2 to 1.8
- latent_frames: bfloat16 [8, 64, 160, 384], P(('groups', 'role'), 'seq'), parts along dimension 0, may hold values from -6 to 6
- frame_cache: bfloat16 [4, 64, 160, 384], P('groups', 'seq'), parts along dimension 0, may hold values from -6 to 6
- vae_gain: float32 [384], replicated, may hold values from 0.5 to 1.5
- conv_weight: bfloat16 [3, 3, 3, 384, 384], replicated, may hold values from -0.0625 to 0.0625
- conv_bias: float32 [384], replicated, may hold values from -1.5 to 1.5
Outputs:
- attended: bfloat16 [8, 4096, 4096], P(('groups', 'role'), 'seq'), parts along dimension 0
- decoded: bfloat16 [8, 64, 160, 384], P(('groups', 'role'), 'seq'), parts along dimension 0
The draws below stay inside these ranges and needn't reach their ends.
There are 2 independent parts, one for each index of `groups`. The reference program is written for one: setup_inputs(seed, part) draws one part's arguments, and reference() takes and returns one part's arrays. A program takes and returns all parts, laid end to end along the dimension named above; an argument that names none is the same for every part. Nothing has to cross between parts.
All inputs are finite; a program needn't handle non-finite values.
Results may differ from the reference program's by a relative error of at most 0.0025.
The reference program's roundings to bfloat16 on the way count: a program that leaves them out, or rounds other values in their place, can miss the bound.
Values may be sent and summed in bfloat16 or wider, within the bound.
A program may use at most 128 MiB of HBM per device.

```python
import math
import jax
import jax.numpy as jnp
from jax import lax

HEADS = 32
HEAD_DIM = 128
CHANNELS = 384
COLS = 160
TOKENS = 4096
SAMPLES = 4
FRAMES = 4
ROWS = 64


def scaled_normal(key):
    width = HEADS * HEAD_DIM
    base = jnp.clip(jax.random.normal(jax.random.fold_in(key, 1), (SAMPLES, TOKENS, width), jnp.float32), -5.0, 5.0)
    row_scale = jnp.exp(jax.random.uniform(jax.random.fold_in(key, 2), (SAMPLES, TOKENS, 1), jnp.float32, 0.0, jnp.log(10.0)))
    col_scale = jnp.exp(jax.random.uniform(jax.random.fold_in(key, 3), (1, 1, width), jnp.float32, 0.0, jnp.log(10.0)))
    return base * row_scale * col_scale


def draw_queries(key, part):
    result = scaled_normal(jax.random.fold_in(key, 11))
    return result.astype(jnp.bfloat16)


def draw_keys(key, part):
    result = scaled_normal(jax.random.fold_in(key, 12))
    return result.astype(jnp.bfloat16)


def shard_levels(own_key, shape, cuts, least, top_value):
    level = 1.0
    for dim, parts in cuts:
        heights = jax.random.uniform(jax.random.fold_in(jax.random.fold_in(own_key, 6), dim), (parts,), jnp.float32, least / len(cuts), top_value / len(cuts))
        level = level * jnp.repeat(jnp.exp(heights), shape[dim] // parts).reshape((-1,) + (1,) * (len(shape) - 1 - dim))
    return level


def centred(own_key, extent, deviation, reach, cuts=(), kind=jnp.bfloat16):
    entries = deviation * jax.random.normal(own_key, extent, jnp.float32)
    if cuts:
        entries = entries * shard_levels(own_key, extent, cuts, -0.22, 0.18)
    return jnp.clip(entries, -reach, reach).astype(kind)


def setup_inputs(seed: int = 0, part: int = 0) -> dict:
    streams_of = jax.random.split(jax.random.key(seed), 11)
    part_splits = jax.random.split(jax.random.fold_in(streams_of[10], part), 11)
    queries = draw_queries(jax.random.fold_in(jax.random.fold_in(streams_of[10], part), 71), part)
    keys = draw_keys(jax.random.fold_in(jax.random.fold_in(streams_of[10], part), 71), part)
    values = centred(part_splits[2], (SAMPLES, TOKENS, HEADS * HEAD_DIM), 1.0, 6.0, ((0, 4), (1, 32)))
    q_gain = jnp.clip(jnp.exp(jax.random.uniform(streams_of[3], (HEADS * HEAD_DIM,), jnp.float32, math.log(1.2), math.log(1.8))), 1.2, 1.8)
    k_gain = jnp.clip(jnp.exp(jax.random.uniform(streams_of[4], (HEADS * HEAD_DIM,), jnp.float32, math.log(1.2), math.log(1.8))), 1.2, 1.8)
    latent_frames = centred(part_splits[5], (FRAMES, ROWS, COLS, CHANNELS), 1.0, 6.0, ((0, 4), (1, 32)))
    frame_cache = centred(part_splits[6], (2, ROWS, COLS, CHANNELS), 1.0, 6.0, ((1, 32),))
    vae_gain = jnp.clip(1.0 + 0.1 * jax.random.normal(streams_of[7], (CHANNELS,), jnp.float32), 0.5, 1.5)
    conv_weight = centred(streams_of[8], (3, 3, 3, CHANNELS, CHANNELS), (27 * CHANNELS) ** -0.5, 0.0625)
    conv_bias = centred(streams_of[9], (CHANNELS,), 0.3, 1.5, (), jnp.float32)
    return dict(queries=queries, keys=keys, values=values, q_gain=q_gain, k_gain=k_gain, latent_frames=latent_frames, frame_cache=frame_cache, vae_gain=vae_gain, conv_weight=conv_weight, conv_bias=conv_bias)


EPSILON = 1e-06

def rms_scale(rows, gain):
    values_f = rows.astype(jnp.float32)
    mean_sq = lax.optimization_barrier(jnp.mean(values_f * values_f, axis=-1, keepdims=True))
    return values_f * lax.rsqrt(mean_sq + EPSILON) * gain.astype(jnp.float32)

def head_attention(triple):
    q_head, k_head, v_head = triple
    length = q_head.shape[0]
    block = min(512, length)
    scale = q_head.shape[1] ** (-0.5)
    k_wide = k_head.astype(jnp.float32)
    v_wide = v_head.astype(jnp.float32)

    def one_block(start):
        rows = lax.dynamic_slice_in_dim(q_head, start, block, 0).astype(jnp.float32)
        scores = jnp.einsum('qd,kd->qk', rows, k_wide, precision=lax.Precision.HIGHEST) * scale
        top = lax.optimization_barrier(jnp.max(scores, axis=1, keepdims=True))
        weights = jnp.exp(scores - top)
        total = lax.optimization_barrier(jnp.sum(weights, axis=1, keepdims=True))
        rounded = weights.astype(jnp.bfloat16).astype(jnp.float32)
        mixed = jnp.dot(rounded, v_wide, precision=lax.Precision.HIGHEST) / total
        return mixed.astype(jnp.bfloat16)
    starts = jnp.arange(length // block, dtype=jnp.int32) * block
    return lax.map(one_block, starts).reshape(length, -1)

def reference(queries, keys, values, q_gain, k_gain, latent_frames, frame_cache, vae_gain, conv_weight, conv_bias):
    samples, tokens, width = queries.shape
    heads = HEADS
    depth = width // heads
    q_normed = rms_scale(queries, q_gain).astype(jnp.bfloat16)
    k_normed = rms_scale(keys, k_gain).astype(jnp.bfloat16)

    def by_head(array):
        return jnp.transpose(array.reshape(samples, tokens, heads, depth), (0, 2, 1, 3)).reshape(samples * heads, tokens, depth)
    outputs = lax.map(head_attention, (by_head(q_normed), by_head(k_normed), by_head(values)))
    attended = jnp.transpose(outputs.reshape(samples, heads, tokens, depth), (0, 2, 1, 3)).reshape(samples, tokens, width)
    joined = jnp.concatenate([frame_cache, latent_frames], axis=0)
    activated = jax.nn.silu(rms_scale(joined, vae_gain)).astype(jnp.bfloat16)
    padded = jnp.pad(activated, ((0, 0), (1, 1), (1, 1), (0, 0)))
    rows = latent_frames.shape[1]
    cols = latent_frames.shape[2]
    chans = latent_frames.shape[3]
    weight = conv_weight.reshape(27 * chans, chans).astype(jnp.float32)

    def one_frame(index):
        window = lax.dynamic_slice_in_dim(padded, index, 3, 0)
        pieces = []
        for a in range(3):
            for b in range(3):
                for e in range(3):
                    pieces.append(window[a, b:b + rows, e:e + cols, :])
        columns = jnp.concatenate(pieces, axis=-1).reshape(rows * cols, 27 * chans).astype(jnp.float32)
        return jnp.dot(columns, weight, precision=lax.Precision.HIGHEST).reshape(rows, cols, chans)
    conv = lax.map(one_frame, jnp.arange(latent_frames.shape[0], dtype=jnp.int32))
    decoded = (latent_frames.astype(jnp.float32) + conv + conv_bias).astype(jnp.bfloat16)
    return (attended, decoded)
```

```python
import functools

import jax
import jax.numpy as jnp
from jax import lax
from jax.experimental import pallas as pl
from jax.experimental.pallas import tpu as pltpu
from jax.sharding import PartitionSpec as P

HEAD_DIM = 128
SEQ = "seq"
MESH = pl.DeviceIdType.MESH
LOG2_E = 1.4426950408889634


EPSILON = 1e-06


def from_behind(value, axis, steps):
    count = lax.axis_size(axis)
    leading, last = (max(0, -steps), min(count, count - steps))
    return lax.ppermute(value, axis, [(source, source + steps) for source in range(leading, last)])


def extended(block, axis, dim, width):
    count = lax.axis_size(axis)
    forward = [(i, i + 1) for i in range(count - 1)]
    backward = [(target, source) for source, target in forward]
    low = lax.ppermute(
        lax.slice_in_dim(block, block.shape[dim] - width, None, axis=dim), axis, forward
    )
    high = lax.ppermute(lax.slice_in_dim(block, 0, width, axis=dim), axis, backward)
    return jnp.concatenate([low, block, high], axis=dim)


def rms_scale(rows, gain):
    values_f = rows.astype(jnp.float32)
    mean_sq = jnp.mean(values_f * values_f, axis=-1, keepdims=True)
    return values_f * lax.rsqrt(mean_sq + EPSILON) * gain


def history(own, past, place):
    before = from_behind(own, "role", 1)
    earlier = from_behind(own, "role", 2)
    one_back = jnp.where(place >= 1, before, past[1:2])
    two_back = jnp.where(place >= 2, earlier, jnp.where(place >= 1, past[1:2], past[0:1]))
    return jnp.concatenate([two_back, one_back, own], axis=0)


def attention_kernel(
    count,
    q_in,
    k_in,
    v_in,
    q_gain,
    k_gain,
    out,
    q_raw,
    k_raw,
    v_raw,
    q_send,
    k_send,
    q_all,
    k_all,
    v_all,
    mixed,
    scores,
    load_sem,
    local_sem,
    send_sem,
    v_sem,
    k_sem,
    q_sem,
    o_sem,
    wave_sem,
):
    chips = count // 2
    half = chips // 2
    rows, width = q_raw.shape
    depth = width // count
    length = rows * count
    me = lax.axis_index(SEQ)
    chip, core = me // 2, me % 2

    def at(offset, other):
        return lax.rem(chip + offset + chips, chips) * 2 + lax.rem(core + other, 2)

    loads = [
        pltpu.make_async_copy(source, target, load_sem.at[i])
        for i, (source, target) in enumerate(((v_in, v_raw), (k_in, k_raw), (q_in, q_raw)))
    ]
    for load in loads:
        load.start()

    barrier = pltpu.get_barrier_semaphore()
    near = [at(0, 1), at(1, 0), at(1, 1), at(-1, 0), at(-1, 1)]
    for device in near:
        pl.semaphore_signal(barrier, inc=1, device_id={SEQ: device}, device_id_type=MESH)
    pl.semaphore_wait(barrier, len(near))

    def columns(head):
        return pl.ds(pl.multiple_of(head * depth, depth), depth)

    def to(device, source, target, sem, arrival):
        pltpu.make_async_remote_copy(
            src_ref=source,
            dst_ref=target,
            send_sem=sem,
            recv_sem=arrival,
            device_id={SEQ: device},
            device_id_type=MESH,
        ).start()

    def send_v(device):
        to(device, v_raw.at[:, columns(device)], v_all.at[me], send_sem.at[0], v_sem)

    def send_k(device):
        to(device, k_send.at[device], k_all.at[me], send_sem.at[1], k_sem)

    def send_q(device):
        to(device, q_send.at[device], q_all.at[me], send_sem.at[2], q_sem.at[me])

    loads[0].wait()
    own_v = pltpu.make_async_copy(v_raw.at[:, columns(me)], v_all.at[me], local_sem.at[0])
    own_v.start()
    send_v(at(0, 1))

    for d in range(1, half + 1):
        if d > 1:
            for device in near[1:]:
                pl.semaphore_signal(
                    wave_sem.at[d - 2], inc=1, device_id={SEQ: device}, device_id_type=MESH
                )
            pl.semaphore_wait(wave_sem.at[d - 2], len(near) - 1)
        for other in range(2):
            send_v(at(d, other))
            if d < half:
                send_v(at(-d, other))

    def normalize(raw, gain, target):
        step = 16

        def some(i, carry):
            at_rows = pl.ds(pl.multiple_of(i * step, step), step)
            wide = raw[at_rows, :].astype(jnp.float32)
            mean_sq = jnp.mean(wide * wide, axis=-1, keepdims=True)
            scaled = (wide * lax.rsqrt(mean_sq + EPSILON) * gain[...]).astype(jnp.bfloat16)
            for head in range(count):
                target[head, at_rows, :] = scaled[:, head * depth : (head + 1) * depth]
            return carry

        lax.fori_loop(0, rows // step, some, 0)

    def send_all(send):
        send(at(0, 1))

        def pair(d, carry):
            for other in range(2):
                send(at(d, other))
                send(at(-d, other))
            return carry

        lax.fori_loop(1, half, pair, 0)
        for other in range(2):
            send(at(half, other))

    loads[1].wait()
    normalize(k_raw, k_gain, k_send)
    own_k = pltpu.make_async_copy(k_send.at[me], k_all.at[me], local_sem.at[1])
    own_k.start()
    send_all(send_k)

    loads[2].wait()
    normalize(q_raw, q_gain, q_send)
    own_q = pltpu.make_async_copy(q_send.at[me], q_all.at[me], local_sem.at[2])
    own_q.start()
    send_all(send_q)

    def arrived(buffer, sem, blocks):
        pltpu.make_async_copy(buffer.at[pl.ds(0, blocks)], buffer.at[pl.ds(0, blocks)], sem).wait()

    own_v.wait()
    own_k.wait()
    own_q.wait()
    arrived(v_all, v_sem, count - 1)
    arrived(k_all, k_sem, count - 1)

    tile = 512
    blocks = tile // rows
    factor = LOG2_E * depth ** (-0.5)
    both = 2 * rows

    def attend(first):
        queries = q_all[pl.ds(first, 2)].reshape(both, depth)
        top = None
        for j in range(length // tile):
            keys = k_all[pl.ds(j * blocks, blocks)].reshape(tile, depth)
            part = lax.dot_general(
                queries, keys, (((1,), (1,)), ((), ())), preferred_element_type=jnp.float32
            )
            scores[:, pl.ds(j * tile, tile)] = part
            for g in range(tile // depth):
                piece = part[:, g * depth : (g + 1) * depth]
                top = piece if top is None else jnp.maximum(top, piece)
        top = jnp.max(top, axis=1, keepdims=True)
        total = jnp.zeros((both, depth), jnp.float32)
        result = jnp.zeros((both, depth), jnp.float32)
        for j in range(length // tile):
            weights = jnp.exp2((scores[:, pl.ds(j * tile, tile)] - top) * factor)
            for g in range(tile // depth):
                total = total + weights[:, g * depth : (g + 1) * depth]
            some_v = v_all[pl.ds(j * blocks, blocks)].reshape(tile, depth)
            result = result + jnp.dot(
                weights.astype(jnp.bfloat16), some_v, preferred_element_type=jnp.float32
            )
        result = result / jnp.sum(total, axis=1, keepdims=True)
        mixed[pl.ds(first, 2)] = result.astype(jnp.bfloat16).reshape(2, rows, depth)

    def send_o(device):
        to(device, mixed.at[device], out.at[me], send_sem.at[3], o_sem)

    def q_arrived(device):
        pltpu.make_async_copy(q_all.at[device], q_all.at[device], q_sem.at[device]).wait()

    q_arrived(at(0, 1))
    attend(chip * 2)
    own_o = pltpu.make_async_copy(mixed.at[me], out.at[me], local_sem.at[3])
    own_o.start()
    send_o(at(0, 1))

    def chip_step(k, carry):
        offset = (k + 1) // 2 * (2 * (k % 2) - 1)
        first = at(offset, 0) // 2 * 2
        q_arrived(first)
        q_arrived(first + 1)
        attend(first)
        send_o(first)
        send_o(first + 1)
        return carry

    lax.fori_loop(1, chips, chip_step, 0)

    own_o.wait()
    arrived(out, o_sem, count - 1)
    arrived(v_all, send_sem.at[0], count - 1)
    arrived(k_all, send_sem.at[1], count - 1)
    arrived(q_all, send_sem.at[2], count - 1)
    arrived(mixed, send_sem.at[3], count - 1)


def attention(queries, keys, values, q_gain, k_gain):
    count = lax.axis_size(SEQ)
    rows, width = queries.shape
    depth = width // count
    blocks = (count, rows, depth)
    anywhere = pl.BlockSpec(memory_space=pl.ANY)
    in_vmem = pl.BlockSpec(memory_space=pltpu.VMEM)
    low = jnp.bfloat16
    return pl.pallas_call(
        functools.partial(attention_kernel, count),
        out_shape=jax.ShapeDtypeStruct(blocks, low),
        in_specs=[anywhere, anywhere, anywhere, in_vmem, in_vmem],
        out_specs=anywhere,
        scratch_shapes=[
            pltpu.VMEM((rows, width), low),
            pltpu.VMEM((rows, width), low),
            pltpu.VMEM((rows, width), low),
            pltpu.VMEM(blocks, low),
            pltpu.VMEM(blocks, low),
            pltpu.VMEM(blocks, low),
            pltpu.VMEM(blocks, low),
            pltpu.VMEM(blocks, low),
            pltpu.VMEM(blocks, low),
            pltpu.VMEM((2 * rows, rows * count), jnp.float32),
            pltpu.SemaphoreType.DMA((3,)),
            pltpu.SemaphoreType.DMA((4,)),
            pltpu.SemaphoreType.DMA((4,)),
            pltpu.SemaphoreType.DMA,
            pltpu.SemaphoreType.DMA,
            pltpu.SemaphoreType.DMA((count,)),
            pltpu.SemaphoreType.DMA,
            pltpu.SemaphoreType.REGULAR((count // 4 - 1,)),
        ],
        compiler_params=pltpu.CompilerParams(
            collective_id=0, has_side_effects=True, vmem_limit_bytes=40 * 1024 * 1024
        ),
        cost_estimate=pl.CostEstimate(
            flops=4 * (rows * count) ** 2 * depth,
            bytes_accessed=8 * rows * width,
            transcendentals=(rows * count) ** 2,
        ),
    )(queries, keys, values, q_gain.reshape(1, width), k_gain.reshape(1, width))


def body(
    queries,
    keys,
    values,
    q_gain,
    k_gain,
    latent_frames,
    frame_cache,
    vae_gain,
    conv_weight,
    conv_bias,
):
    tok_local = queries.shape[1]
    width = queries.shape[2]
    activated_own = jax.nn.silu(rms_scale(latent_frames, vae_gain)).astype(jnp.bfloat16)
    activated_past = jax.nn.silu(rms_scale(frame_cache, vae_gain)).astype(jnp.bfloat16)
    place = lax.axis_index("role")
    stacked = history(activated_own, activated_past, place)
    stacked = extended(stacked, SEQ, 1, 1)
    stacked = jnp.pad(stacked, ((0, 0), (0, 0), (1, 1), (0, 0)))
    rows = latent_frames.shape[1]
    cols = latent_frames.shape[2]
    chans = latent_frames.shape[3]
    pieces = []
    for a in range(3):
        for b in range(3):
            for e in range(3):
                pieces.append(stacked[a, b : b + rows, e : e + cols, :])
    columns = jnp.concatenate(pieces, axis=-1).reshape(rows * cols, 27 * chans)
    weight = conv_weight.reshape(27 * chans, chans)
    conv = jnp.dot(columns, weight, preferred_element_type=jnp.float32).reshape(
        1, rows, cols, chans
    )
    decoded = (latent_frames.astype(jnp.float32) + conv + conv_bias).astype(jnp.bfloat16)
    blocks = attention(queries[0], keys[0], values[0], q_gain, k_gain)
    attended = jnp.moveaxis(blocks, 0, 1).reshape(1, tok_local, width)
    return (attended, decoded)


def solution(mesh):
    in_specs = (
        P(("groups", "role"), SEQ, None),
        P(("groups", "role"), SEQ, None),
        P(("groups", "role"), SEQ, None),
        P(),
        P(),
        P(("groups", "role"), SEQ, None, None),
        P("groups", SEQ, None, None),
        P(),
        P(),
        P(),
    )
    out_specs = (P(("groups", "role"), SEQ, None), P(("groups", "role"), SEQ, None, None))
    return jax.shard_map(body, mesh=mesh, in_specs=in_specs, out_specs=out_specs, check_vma=False)
```

```python
import functools

import jax
import jax.numpy as jnp
from jax import lax
from jax.experimental import pallas as pl
from jax.experimental.pallas import tpu as pltpu
from jax.sharding import PartitionSpec as P

HEAD_DIM = 128
SEQ = "seq"
ROLE = "role"
MESH = pl.DeviceIdType.MESH
VMEM_BYTES = 67043328
LOG2_E = 1.4426950408889634


EPSILON = 1e-06


def block_kernel(
    count,
    roles,
    q_in,
    k_in,
    v_in,
    q_gain_in,
    k_gain_in,
    latent_in,
    cache_in,
    vae_gain_in,
    weight_in,
    bias_in,
    out,
    decoded_out,
    q_raw,
    k_raw,
    v_raw,
    q_gain,
    k_gain,
    latent,
    cache,
    vae_gain,
    weight,
    bias,
    frames,
    past,
    past_halo,
    sums,
    decoded,
    q_send,
    k_send,
    q_all,
    k_all,
    v_all,
    mixed,
    scores,
    load_sem,
    local_sem,
    send_sem,
    v_sem,
    k_sem,
    q_sem,
    o_sem,
    wave_sem,
    halo_send,
    halo_sem,
    frame_send,
    frame_sem,
    piece_send,
    piece_sem,
):
    chips = count // 2
    half = chips // 2
    rows, width = q_raw.shape
    depth = width // count
    length = rows * count
    me = lax.axis_index(SEQ)
    chip, core = me // 2, me % 2
    role = lax.axis_index(ROLE)
    image_rows, cols, chans = latent.shape
    pasts = cache.shape[0]
    shares = roles // pasts
    share = cols // shares
    last = image_rows + 1

    def at(offset, other):
        return lax.rem(chip + offset + chips, chips) * 2 + lax.rem(core + other, 2)

    loads = [
        pltpu.make_async_copy(source, target, load_sem.at[i])
        for i, (source, target) in enumerate(
            (
                (v_in, v_raw),
                (latent_in, latent),
                (cache_in, cache),
                (vae_gain_in, vae_gain),
                (k_in, k_raw),
                (k_gain_in, k_gain),
                (q_in, q_raw),
                (q_gain_in, q_gain),
                (weight_in, weight),
                (bias_in, bias),
            )
        )
    ]
    v_load, latent_load, cache_load, vae_gain_load = loads[:4]
    k_load, k_gain_load, q_load, q_gain_load, weight_load, bias_load = loads[4:]
    for load in loads:
        load.start()

    barrier = pltpu.get_barrier_semaphore()
    near = [at(0, 1), at(1, 0), at(1, 1), at(-1, 0), at(-1, 1)]
    for device in near:
        pl.semaphore_signal(barrier, inc=1, device_id={SEQ: device}, device_id_type=MESH)
    for step in range(1, roles):
        pl.semaphore_signal(
            barrier,
            inc=1,
            device_id={ROLE: lax.rem(role + step, roles)},
            device_id_type=MESH,
        )
    pl.semaphore_wait(barrier, len(near) + roles - 1)

    def columns(head):
        return pl.ds(pl.multiple_of(head * depth, depth), depth)

    def to(device, source, target, sem, arrival):
        pltpu.make_async_remote_copy(
            src_ref=source,
            dst_ref=target,
            send_sem=sem,
            recv_sem=arrival,
            device_id={SEQ: device},
            device_id_type=MESH,
        ).start()

    def send_v(device):
        to(device, v_raw.at[:, columns(device)], v_all.at[me], send_sem.at[0], v_sem)

    def send_k(device):
        to(device, k_send.at[device], k_all.at[me], send_sem.at[1], k_sem)

    def send_q(device):
        to(device, q_send.at[device], q_all.at[me], send_sem.at[2], q_sem.at[me])

    v_load.wait()
    own_v = pltpu.make_async_copy(v_raw.at[:, columns(me)], v_all.at[me], local_sem.at[0])
    own_v.start()
    send_v(at(0, 1))

    def activated(values):
        wide = values.astype(jnp.float32)
        mean_sq = jnp.mean(wide * wide, axis=-1, keepdims=True)
        scaled = wide * lax.rsqrt(mean_sq + EPSILON) * vae_gain[...].reshape(1, chans)
        return (scaled * lax.logistic(scaled)).astype(jnp.bfloat16)

    def activate():
        latent_load.wait()
        cache_load.wait()
        vae_gain_load.wait()
        for row in range(image_rows):
            frames[2, 1 + row] = activated(latent[row])
            for frame in range(pasts):
                past[frame, row] = activated(cache[frame, row])

        @pl.when(me == 0)
        def _():
            frames[2, 0] = jnp.zeros((cols, chans), frames.dtype)
            past_halo[0] = jnp.zeros((share, chans), past_halo.dtype)

        @pl.when(me == count - 1)
        def _():
            frames[2, last] = jnp.zeros((cols, chans), frames.dtype)
            past_halo[1] = jnp.zeros((share, chans), past_halo.dtype)

    my_past = role // shares
    my_cols = pl.ds(pl.multiple_of(lax.rem(role, shares) * share, share), share)

    def halo_copies(device, side):
        edge = 0 if side == 0 else image_rows - 1
        landing = 1 - side
        pairs = (
            (frames.at[2, 1 + edge], frames.at[2, landing * last]),
            (past.at[my_past, edge, my_cols], past_halo.at[landing]),
        )
        return [
            pltpu.make_async_remote_copy(
                src_ref=source,
                dst_ref=target,
                send_sem=halo_send.at[side, i],
                recv_sem=halo_sem.at[landing, i],
                device_id={SEQ: device},
                device_id_type=MESH,
            )
            for i, (source, target) in enumerate(pairs)
        ]

    def each_side(act):
        @pl.when(me > 0)
        def _():
            act(me - 1, 0)

        @pl.when(me < count - 1)
        def _():
            act(me + 1, 1)

    def send_halos():
        def start(device, side):
            for copy in halo_copies(device, side):
                copy.start()

        each_side(start)

    def wait_halos():
        def wait(device, side):
            for i, target in enumerate((frames.at[2, side * last], past_halo.at[side])):
                pltpu.make_async_copy(target, target, halo_sem.at[side, i]).wait()

        each_side(wait)

    def frame_copy(ahead):
        return pltpu.make_async_remote_copy(
            src_ref=frames.at[2],
            dst_ref=frames.at[2 - ahead],
            send_sem=frame_send.at[ahead - 1],
            recv_sem=frame_sem.at[ahead - 1],
            device_id={ROLE: role + ahead},
            device_id_type=MESH,
        )

    def piece_place(frame, target, side, source_role):
        part = pl.ds(pl.multiple_of(lax.rem(source_role, shares) * share, share), share)
        return frames.at[frame - target, side * last, part]

    def pieces(act_remote, act_local):
        for target in range(pasts):
            for frame in range(target, pasts):
                for side in range(2):
                    mine = jnp.logical_and(my_past == frame, role != target)
                    here = jnp.logical_and(my_past == frame, role == target)

                    @pl.when(mine)
                    def _():
                        act_remote(frame, target, side)

                    @pl.when(here)
                    def _():
                        act_local(frame, target, side)

    def piece_copy(frame, target, side):
        return pltpu.make_async_remote_copy(
            src_ref=past_halo.at[side],
            dst_ref=piece_place(frame, target, side, role),
            send_sem=piece_send.at[target, side],
            recv_sem=piece_sem.at[role, side],
            device_id={ROLE: target},
            device_id_type=MESH,
        )

    def own_piece(frame, target, side):
        return pltpu.make_async_copy(
            past_halo.at[side],
            piece_place(frame, target, side, role),
            piece_send.at[target, side],
        )

    def pass_on():
        for ahead in (1, 2):

            @pl.when(role + ahead < roles)
            def _():
                frame_copy(ahead).start()

        pieces(
            lambda *which: piece_copy(*which).start(), lambda *which: own_piece(*which).start()
        )
        for target in range(pasts):

            @pl.when(role == target)
            def _():
                for frame in range(target, pasts):
                    frames[frame - target, 1 : 1 + image_rows] = past[frame]

    def wait_frames():
        for ahead in (1, 2):

            @pl.when(role >= ahead)
            def _():
                target = frames.at[2 - ahead]
                pltpu.make_async_copy(target, target, frame_sem.at[ahead - 1]).wait()

        for target in range(pasts):

            @pl.when(role == target)
            def _():
                for source_role in range(target * shares, roles):
                    if source_role == target:
                        continue
                    for side in range(2):
                        place = piece_place(source_role // shares, target, side, source_role)
                        pltpu.make_async_copy(place, place, piece_sem.at[source_role, side]).wait()

        pieces(lambda *which: None, lambda *which: own_piece(*which).wait())

    def wait_conv_sends():
        def wait(device, side):
            for copy in halo_copies(device, side):
                copy.wait_send()

        each_side(wait)
        for ahead in (1, 2):

            @pl.when(role + ahead < roles)
            def _():
                frame_copy(ahead).wait_send()

        pieces(lambda *which: piece_copy(*which).wait_send(), lambda *which: None)

    def convolve():
        flat = image_rows * cols
        sums[...] = jnp.zeros_like(sums)

        def tap(i, carry):
            a, b = i // 3, i % 3
            window = frames[a, pl.ds(b, image_rows)].reshape(flat, chans)
            for e in range(3):
                sums[e] += jnp.dot(window, weight[a, b, e], preferred_element_type=jnp.float32)
            return carry

        lax.fori_loop(0, 9, tap, 0)
        index = lax.broadcasted_iota(jnp.int32, (cols, chans), 0)
        for row in range(image_rows):
            part = pl.ds(row * cols, cols)
            left = jnp.where(index == 0, 0.0, pltpu.roll(sums[0, part], 1, 0))
            right = jnp.where(index == cols - 1, 0.0, pltpu.roll(sums[2, part], cols - 1, 0))
            conv = sums[1, part] + left + right
            decoded[row] = (latent[row].astype(jnp.float32) + conv + bias[...].reshape(1, chans)).astype(
                decoded.dtype
            )

    for d in range(1, half + 1):
        if d > 1:
            for device in near[1:]:
                pl.semaphore_signal(
                    wave_sem.at[d - 2], inc=1, device_id={SEQ: device}, device_id_type=MESH
                )
            pl.semaphore_wait(wave_sem.at[d - 2], len(near) - 1)
        for other in range(2):
            send_v(at(d, other))
            if d < half:
                send_v(at(-d, other))
        if d == 2:
            activate()
            send_halos()

    def normalize(raw, gain, target):
        step = 16

        def some(i, carry):
            at_rows = pl.ds(pl.multiple_of(i * step, step), step)
            wide = raw[at_rows, :].astype(jnp.float32)
            mean_sq = jnp.mean(wide * wide, axis=-1, keepdims=True)
            scaled = (wide * lax.rsqrt(mean_sq + EPSILON) * gain[...]).astype(jnp.bfloat16)
            for head in range(count):
                target[head, at_rows, :] = scaled[:, head * depth : (head + 1) * depth]
            return carry

        lax.fori_loop(0, rows // step, some, 0)

    def send_all(send):
        send(at(0, 1))

        def pair(d, carry):
            for other in range(2):
                send(at(d, other))
                send(at(-d, other))
            return carry

        lax.fori_loop(1, half, pair, 0)
        for other in range(2):
            send(at(half, other))

    k_load.wait()
    k_gain_load.wait()
    normalize(k_raw, k_gain, k_send)
    own_k = pltpu.make_async_copy(k_send.at[me], k_all.at[me], local_sem.at[1])
    own_k.start()
    send_all(send_k)

    q_load.wait()
    q_gain_load.wait()
    normalize(q_raw, q_gain, q_send)
    own_q = pltpu.make_async_copy(q_send.at[me], q_all.at[me], local_sem.at[2])
    own_q.start()

    def farthest_first(i, carry):
        d = half - i
        for other in range(2):
            send_q(at(d, other))
            send_q(at(-d, other))
        return carry

    for other in range(2):
        send_q(at(half, other))
    lax.fori_loop(1, half, farthest_first, 0)
    send_q(at(0, 1))

    wait_halos()
    pass_on()
    weight_load.wait()
    bias_load.wait()
    wait_frames()
    convolve()
    decoded_store = pltpu.make_async_copy(decoded, decoded_out, local_sem.at[4])
    decoded_store.start()

    def arrived(buffer, sem, blocks):
        pltpu.make_async_copy(buffer.at[pl.ds(0, blocks)], buffer.at[pl.ds(0, blocks)], sem).wait()

    own_v.wait()
    own_k.wait()
    own_q.wait()
    arrived(v_all, v_sem, count - 1)
    arrived(k_all, k_sem, count - 1)

    tile = 512
    blocks = tile // rows
    factor = LOG2_E * depth ** (-0.5)
    both = 2 * rows

    def attend(first):
        queries = q_all[pl.ds(first, 2)].reshape(both, depth)
        top = None
        for j in range(length // tile):
            keys = k_all[pl.ds(j * blocks, blocks)].reshape(tile, depth)
            part = lax.dot_general(
                queries, keys, (((1,), (1,)), ((), ())), preferred_element_type=jnp.float32
            )
            scores[:, pl.ds(j * tile, tile)] = part
            for g in range(tile // depth):
                piece = part[:, g * depth : (g + 1) * depth]
                top = piece if top is None else jnp.maximum(top, piece)
        top = jnp.max(top, axis=1, keepdims=True)
        total = jnp.zeros((both, depth), jnp.float32)
        result = jnp.zeros((both, depth), jnp.float32)
        for j in range(length // tile):
            weights = jnp.exp2((scores[:, pl.ds(j * tile, tile)] - top) * factor)
            for g in range(tile // depth):
                total = total + weights[:, g * depth : (g + 1) * depth]
            some_v = v_all[pl.ds(j * blocks, blocks)].reshape(tile, depth)
            result = result + jnp.dot(
                weights.astype(jnp.bfloat16), some_v, preferred_element_type=jnp.float32
            )
        result = result / jnp.sum(total, axis=1, keepdims=True)
        mixed[pl.ds(first, 2)] = result.astype(jnp.bfloat16).reshape(2, rows, depth)

    def send_o(device):
        to(device, mixed.at[device], out.at[:, columns(me)], send_sem.at[3], o_sem)

    def q_arrived(device):
        pltpu.make_async_copy(q_all.at[device], q_all.at[device], q_sem.at[device]).wait()

    q_arrived(at(0, 1))
    attend(chip * 2)
    own_o = pltpu.make_async_copy(mixed.at[me], out.at[:, columns(me)], local_sem.at[3])
    own_o.start()
    send_o(at(0, 1))

    def chip_step(k, carry):
        j = chips - k
        offset = (j + 1) // 2 * (2 * (j % 2) - 1)
        first = at(offset, 0) // 2 * 2
        q_arrived(first)
        q_arrived(first + 1)
        attend(first)
        send_o(first)
        send_o(first + 1)
        return carry

    lax.fori_loop(1, chips, chip_step, 0)

    wait_conv_sends()
    decoded_store.wait()
    own_o.wait()
    arrived(mixed, o_sem, count - 1)
    arrived(v_all, send_sem.at[0], count - 1)
    arrived(k_all, send_sem.at[1], count - 1)
    arrived(q_all, send_sem.at[2], count - 1)
    arrived(mixed, send_sem.at[3], count - 1)


def store_kernel(attended, decoded, attended_out, decoded_out, wide, image, load_sem, store_sem):
    pieces = load_sem.shape[0] - 1
    step = wide.shape[0] // pieces
    moves = [(decoded, image, decoded_out)]
    for i in range(pieces):
        part = pl.ds(i * step, step)
        moves.append((attended.at[part], wide.at[part], attended_out.at[part]))
    loads = [pltpu.make_async_copy(m[0], m[1], load_sem.at[i]) for i, m in enumerate(moves)]
    stores = [pltpu.make_async_copy(m[1], m[2], store_sem.at[i]) for i, m in enumerate(moves)]
    for load in loads:
        load.start()
    for load, store in zip(loads, stores):
        load.wait()
        store.start()
    for store in stores:
        store.wait()


def body(
    queries,
    keys,
    values,
    q_gain,
    k_gain,
    latent_frames,
    frame_cache,
    vae_gain,
    conv_weight,
    conv_bias,
):
    count, roles = lax.axis_size(SEQ), lax.axis_size(ROLE)
    _, rows, width = queries.shape
    depth = HEAD_DIM
    pasts = frame_cache.shape[0]
    _, image_rows, cols, chans = latent_frames.shape
    blocks = (count, rows, depth)
    in_hbm = pl.BlockSpec(memory_space=pltpu.HBM)
    anywhere = pl.BlockSpec(memory_space=pl.ANY)
    low, wide = jnp.bfloat16, jnp.float32
    dma = pltpu.SemaphoreType.DMA
    attended, decoded = pl.pallas_call(
        functools.partial(block_kernel, count, roles),
        out_shape=(
            jax.ShapeDtypeStruct((rows, width), low),
            jax.ShapeDtypeStruct((image_rows, cols, chans), low),
        ),
        in_specs=[in_hbm] * 10,
        out_specs=(anywhere, anywhere),
        scratch_shapes=[
            pltpu.VMEM((rows, width), low),
            pltpu.VMEM((rows, width), low),
            pltpu.VMEM((rows, width), low),
            pltpu.VMEM((1, width), wide),
            pltpu.VMEM((1, width), wide),
            pltpu.VMEM((image_rows, cols, chans), low),
            pltpu.VMEM((pasts, image_rows, cols, chans), low),
            pltpu.VMEM((chans,), wide),
            pltpu.VMEM(conv_weight.shape, low),
            pltpu.VMEM((chans,), wide),
            pltpu.VMEM((3, image_rows + 2, cols, chans), low),
            pltpu.VMEM((pasts, image_rows, cols, chans), low),
            pltpu.VMEM((2, cols * pasts // roles, chans), low),
            pltpu.VMEM((3, image_rows * cols, chans), wide),
            pltpu.VMEM((image_rows, cols, chans), low),
            pltpu.VMEM(blocks, low),
            pltpu.VMEM(blocks, low),
            pltpu.VMEM(blocks, low),
            pltpu.VMEM(blocks, low),
            pltpu.VMEM(blocks, low),
            pltpu.VMEM(blocks, low),
            pltpu.VMEM((2 * rows, rows * count), wide),
            dma((10,)),
            dma((5,)),
            dma((4,)),
            dma,
            dma,
            dma((count,)),
            dma,
            pltpu.SemaphoreType.REGULAR((count // 4 - 1,)),
            dma((2, 2)),
            dma((2, 2)),
            dma((2,)),
            dma((2,)),
            dma((pasts, 2)),
            dma((roles, 2)),
        ],
        compiler_params=pltpu.CompilerParams(
            collective_id=0, has_side_effects=True, vmem_limit_bytes=VMEM_BYTES
        ),
    )(
        queries[0],
        keys[0],
        values[0],
        q_gain.reshape(1, width),
        k_gain.reshape(1, width),
        latent_frames[0],
        frame_cache,
        vae_gain,
        conv_weight,
        conv_bias,
    )
    attended, decoded = pl.pallas_call(
        store_kernel,
        out_shape=(
            jax.ShapeDtypeStruct((rows, width), low),
            jax.ShapeDtypeStruct((image_rows, cols, chans), low),
        ),
        in_specs=[anywhere] * 2,
        out_specs=(anywhere, anywhere),
        scratch_shapes=[
            pltpu.VMEM((rows, width), low),
            pltpu.VMEM((image_rows, cols, chans), low),
            dma((5,)),
            dma((5,)),
        ],
        compiler_params=pltpu.CompilerParams(vmem_limit_bytes=VMEM_BYTES),
    )(attended, decoded)
    return attended[None], decoded[None]


def solution(mesh):
    in_specs = (
        P(("groups", "role"), SEQ, None),
        P(("groups", "role"), SEQ, None),
        P(("groups", "role"), SEQ, None),
        P(),
        P(),
        P(("groups", "role"), SEQ, None, None),
        P("groups", SEQ, None, None),
        P(),
        P(),
        P(),
    )
    out_specs = (P(("groups", "role"), SEQ, None), P(("groups", "role"), SEQ, None, None))
    return jax.shard_map(body, mesh=mesh, in_specs=in_specs, out_specs=out_specs, check_vma=False)
```

```python
import functools

import jax
import jax.numpy as jnp
from jax import lax
from jax.experimental import pallas as pl
from jax.experimental.pallas import tpu as pltpu
from jax.sharding import PartitionSpec as P

HEAD_DIM = 128
SEQ = "seq"
ROLE = "role"
MESH = pl.DeviceIdType.MESH
VMEM_BYTES = 67043328
LOG2_E = 1.4426950408889634


EPSILON = 1e-06


def block_kernel(
    count,
    roles,
    q_in,
    k_in,
    v_in,
    q_gain_in,
    k_gain_in,
    latent_in,
    cache_in,
    vae_gain_in,
    weight_in,
    bias_in,
    out,
    decoded_out,
    q_raw,
    k_raw,
    v_raw,
    q_gain,
    k_gain,
    latent,
    cache,
    vae_gain,
    weight,
    bias,
    frames,
    past,
    past_halo,
    sums,
    decoded,
    q_send,
    k_send,
    q_all,
    k_all,
    v_all,
    mixed,
    scores,
    load_sem,
    local_sem,
    send_sem,
    v_sem,
    k_sem,
    q_sem,
    o_sem,
    wave_sem,
    halo_send,
    halo_sem,
    frame_send,
    frame_sem,
    piece_send,
    piece_sem,
):
    chips = count // 2
    half = chips // 2
    rows, width = q_raw.shape
    depth = width // count
    length = rows * count
    me = lax.axis_index(SEQ)
    chip, core = me // 2, me % 2
    role = lax.axis_index(ROLE)
    image_rows, cols, chans = latent.shape
    pasts = cache.shape[0]
    shares = roles // pasts
    share = cols // shares
    last = image_rows + 1

    def at(offset, other):
        return lax.rem(chip + offset + chips, chips) * 2 + lax.rem(core + other, 2)

    loads = [
        pltpu.make_async_copy(source, target, load_sem.at[i])
        for i, (source, target) in enumerate(
            (
                (v_in, v_raw),
                (latent_in, latent),
                (cache_in, cache),
                (vae_gain_in, vae_gain),
                (k_in, k_raw),
                (k_gain_in, k_gain),
                (q_in, q_raw),
                (q_gain_in, q_gain),
                (weight_in, weight),
                (bias_in, bias),
            )
        )
    ]
    v_load, latent_load, cache_load, vae_gain_load = loads[:4]
    k_load, k_gain_load, q_load, q_gain_load, weight_load, bias_load = loads[4:]
    v_load.start()

    barrier = pltpu.get_barrier_semaphore()
    near = [at(0, 1), at(1, 0), at(1, 1), at(-1, 0), at(-1, 1)]
    for device in near:
        pl.semaphore_signal(barrier, inc=1, device_id={SEQ: device}, device_id_type=MESH)
    for step in range(1, roles):
        pl.semaphore_signal(
            barrier,
            inc=1,
            device_id={ROLE: lax.rem(role + step, roles)},
            device_id_type=MESH,
        )
    pl.semaphore_wait(barrier, len(near) + roles - 1)

    def columns(head):
        return pl.ds(pl.multiple_of(head * depth, depth), depth)

    def to(device, source, target, sem, arrival):
        pltpu.make_async_remote_copy(
            src_ref=source,
            dst_ref=target,
            send_sem=sem,
            recv_sem=arrival,
            device_id={SEQ: device},
            device_id_type=MESH,
        ).start()

    def send_v(device):
        to(device, v_raw.at[:, columns(device)], v_all.at[me], send_sem.at[0], v_sem)

    def send_k(device):
        to(device, k_send.at[device], k_all.at[me], send_sem.at[1], k_sem)

    def send_q(device):
        to(device, q_send.at[device], q_all.at[me], send_sem.at[2], q_sem.at[me])

    v_load.wait()
    own_v = pltpu.make_async_copy(v_raw.at[:, columns(me)], v_all.at[me], local_sem.at[0])
    own_v.start()
    send_v(at(0, 1))
    for load in loads[1:-2]:
        load.start()

    def activated(values):
        wide = values.astype(jnp.float32)
        mean_sq = jnp.mean(wide * wide, axis=-1, keepdims=True)
        scaled = wide * lax.rsqrt(mean_sq + EPSILON) * vae_gain[...].reshape(1, chans)
        return (scaled * lax.logistic(scaled)).astype(jnp.bfloat16)

    def activate():
        latent_load.wait()
        cache_load.wait()
        vae_gain_load.wait()
        for row in range(image_rows):
            frames[2, 1 + row] = activated(latent[row])
            for frame in range(pasts):
                past[frame, row] = activated(cache[frame, row])

        @pl.when(me == 0)
        def _():
            frames[2, 0] = jnp.zeros((cols, chans), frames.dtype)
            past_halo[0] = jnp.zeros((share, chans), past_halo.dtype)

        @pl.when(me == count - 1)
        def _():
            frames[2, last] = jnp.zeros((cols, chans), frames.dtype)
            past_halo[1] = jnp.zeros((share, chans), past_halo.dtype)

    my_past = role // shares
    my_cols = pl.ds(pl.multiple_of(lax.rem(role, shares) * share, share), share)

    def halo_copies(device, side):
        edge = 0 if side == 0 else image_rows - 1
        landing = 1 - side
        pairs = (
            (frames.at[2, 1 + edge], frames.at[2, landing * last]),
            (past.at[my_past, edge, my_cols], past_halo.at[landing]),
        )
        return [
            pltpu.make_async_remote_copy(
                src_ref=source,
                dst_ref=target,
                send_sem=halo_send.at[side, i],
                recv_sem=halo_sem.at[landing, i],
                device_id={SEQ: device},
                device_id_type=MESH,
            )
            for i, (source, target) in enumerate(pairs)
        ]

    def each_side(act):
        @pl.when(me > 0)
        def _():
            act(me - 1, 0)

        @pl.when(me < count - 1)
        def _():
            act(me + 1, 1)

    def send_halos():
        def start(device, side):
            for copy in halo_copies(device, side):
                copy.start()

        each_side(start)

    def wait_halos():
        def wait(device, side):
            for i, target in enumerate((frames.at[2, side * last], past_halo.at[side])):
                pltpu.make_async_copy(target, target, halo_sem.at[side, i]).wait()

        each_side(wait)

    def frame_copy(ahead):
        return pltpu.make_async_remote_copy(
            src_ref=frames.at[2],
            dst_ref=frames.at[2 - ahead],
            send_sem=frame_send.at[ahead - 1],
            recv_sem=frame_sem.at[ahead - 1],
            device_id={ROLE: role + ahead},
            device_id_type=MESH,
        )

    def piece_place(frame, target, side, source_role):
        part = pl.ds(pl.multiple_of(lax.rem(source_role, shares) * share, share), share)
        return frames.at[frame - target, side * last, part]

    def pieces(act_remote, act_local):
        for target in range(pasts):
            for frame in range(target, pasts):
                for side in range(2):
                    mine = jnp.logical_and(my_past == frame, role != target)
                    here = jnp.logical_and(my_past == frame, role == target)

                    @pl.when(mine)
                    def _():
                        act_remote(frame, target, side)

                    @pl.when(here)
                    def _():
                        act_local(frame, target, side)

    def piece_copy(frame, target, side):
        return pltpu.make_async_remote_copy(
            src_ref=past_halo.at[side],
            dst_ref=piece_place(frame, target, side, role),
            send_sem=piece_send.at[target, side],
            recv_sem=piece_sem.at[role, side],
            device_id={ROLE: target},
            device_id_type=MESH,
        )

    def own_piece(frame, target, side):
        return pltpu.make_async_copy(
            past_halo.at[side],
            piece_place(frame, target, side, role),
            piece_send.at[target, side],
        )

    def pass_on():
        for ahead in (1, 2):

            @pl.when(role + ahead < roles)
            def _():
                frame_copy(ahead).start()

        pieces(
            lambda *which: piece_copy(*which).start(), lambda *which: own_piece(*which).start()
        )
        for target in range(pasts):

            @pl.when(role == target)
            def _():
                for frame in range(target, pasts):
                    frames[frame - target, 1 : 1 + image_rows] = past[frame]

    def wait_frames():
        for ahead in (1, 2):

            @pl.when(role >= ahead)
            def _():
                target = frames.at[2 - ahead]
                pltpu.make_async_copy(target, target, frame_sem.at[ahead - 1]).wait()

        for target in range(pasts):

            @pl.when(role == target)
            def _():
                for source_role in range(target * shares, roles):
                    if source_role == target:
                        continue
                    for side in range(2):
                        place = piece_place(source_role // shares, target, side, source_role)
                        pltpu.make_async_copy(place, place, piece_sem.at[source_role, side]).wait()

        pieces(lambda *which: None, lambda *which: own_piece(*which).wait())

    def wait_conv_sends():
        def wait(device, side):
            for copy in halo_copies(device, side):
                copy.wait_send()

        each_side(wait)
        for ahead in (1, 2):

            @pl.when(role + ahead < roles)
            def _():
                frame_copy(ahead).wait_send()

        pieces(lambda *which: piece_copy(*which).wait_send(), lambda *which: None)

    def convolve():
        flat = image_rows * cols
        sums[...] = jnp.zeros_like(sums)

        def tap(i, carry):
            a, b = i // 3, i % 3
            window = frames[a, pl.ds(b, image_rows)].reshape(flat, chans)
            for e in range(3):
                sums[e] += jnp.dot(window, weight[a, b, e], preferred_element_type=jnp.float32)
            return carry

        lax.fori_loop(0, 9, tap, 0)
        index = lax.broadcasted_iota(jnp.int32, (cols, chans), 0)
        for row in range(image_rows):
            part = pl.ds(row * cols, cols)
            left = jnp.where(index == 0, 0.0, pltpu.roll(sums[0, part], 1, 0))
            right = jnp.where(index == cols - 1, 0.0, pltpu.roll(sums[2, part], cols - 1, 0))
            conv = sums[1, part] + left + right
            decoded[row] = (latent[row].astype(jnp.float32) + conv + bias[...].reshape(1, chans)).astype(
                decoded.dtype
            )

    for d in range(1, half + 1):
        if d > 1:
            for device in near[1:]:
                pl.semaphore_signal(
                    wave_sem.at[d - 2], inc=1, device_id={SEQ: device}, device_id_type=MESH
                )
            pl.semaphore_wait(wave_sem.at[d - 2], len(near) - 1)
        for other in range(2):
            send_v(at(d, other))
            if d < half:
                send_v(at(-d, other))
        if d == half // 2:
            weight_load.start()
            bias_load.start()
            activate()
            send_halos()

    def normalize(raw, gain, target):
        step = 16

        def some(i, carry):
            at_rows = pl.ds(pl.multiple_of(i * step, step), step)
            wide = raw[at_rows, :].astype(jnp.float32)
            mean_sq = jnp.mean(wide * wide, axis=-1, keepdims=True)
            scaled = (wide * lax.rsqrt(mean_sq + EPSILON) * gain[...]).astype(jnp.bfloat16)
            for head in range(count):
                target[head, at_rows, :] = scaled[:, head * depth : (head + 1) * depth]
            return carry

        lax.fori_loop(0, rows // step, some, 0)

    def send_all(send):
        send(at(0, 1))

        def pair(d, carry):
            for other in range(2):
                send(at(d, other))
                send(at(-d, other))
            return carry

        lax.fori_loop(1, half, pair, 0)
        for other in range(2):
            send(at(half, other))

    k_load.wait()
    k_gain_load.wait()
    normalize(k_raw, k_gain, k_send)
    own_k = pltpu.make_async_copy(k_send.at[me], k_all.at[me], local_sem.at[1])
    own_k.start()
    send_all(send_k)

    q_load.wait()
    q_gain_load.wait()
    normalize(q_raw, q_gain, q_send)
    own_q = pltpu.make_async_copy(q_send.at[me], q_all.at[me], local_sem.at[2])
    own_q.start()

    def farthest_first(i, carry):
        d = half - i
        for other in range(2):
            send_q(at(d, other))
            send_q(at(-d, other))
        return carry

    for other in range(2):
        send_q(at(half, other))
    lax.fori_loop(1, half, farthest_first, 0)
    send_q(at(0, 1))

    wait_halos()
    pass_on()
    weight_load.wait()
    bias_load.wait()
    wait_frames()
    convolve()
    decoded_store = pltpu.make_async_copy(decoded, decoded_out, local_sem.at[4])
    decoded_store.start()

    def arrived(buffer, sem, blocks):
        pltpu.make_async_copy(buffer.at[pl.ds(0, blocks)], buffer.at[pl.ds(0, blocks)], sem).wait()

    own_v.wait()
    own_k.wait()
    own_q.wait()
    arrived(v_all, v_sem, count - 1)
    arrived(k_all, k_sem, count - 1)

    tile = 512
    blocks = tile // rows
    factor = LOG2_E * depth ** (-0.5)
    both = 2 * rows

    def attend(first):
        queries = q_all[pl.ds(first, 2)].reshape(both, depth)
        top = None
        for j in range(length // tile):
            keys = k_all[pl.ds(j * blocks, blocks)].reshape(tile, depth)
            part = lax.dot_general(
                queries, keys, (((1,), (1,)), ((), ())), preferred_element_type=jnp.float32
            )
            scores[:, pl.ds(j * tile, tile)] = part
            for g in range(tile // depth):
                piece = part[:, g * depth : (g + 1) * depth]
                top = piece if top is None else jnp.maximum(top, piece)
        top = jnp.max(top, axis=1, keepdims=True)
        total = jnp.zeros((both, depth), jnp.float32)
        result = jnp.zeros((both, depth), jnp.float32)
        for j in range(length // tile):
            weights = jnp.exp2((scores[:, pl.ds(j * tile, tile)] - top) * factor)
            for g in range(tile // depth):
                total = total + weights[:, g * depth : (g + 1) * depth]
            some_v = v_all[pl.ds(j * blocks, blocks)].reshape(tile, depth)
            result = result + jnp.dot(
                weights.astype(jnp.bfloat16), some_v, preferred_element_type=jnp.float32
            )
        result = result / jnp.sum(total, axis=1, keepdims=True)
        mixed[pl.ds(first, 2)] = result.astype(jnp.bfloat16).reshape(2, rows, depth)

    def send_o(device):
        to(device, mixed.at[device], out.at[:, columns(me)], send_sem.at[3], o_sem)

    def q_arrived(device):
        pltpu.make_async_copy(q_all.at[device], q_all.at[device], q_sem.at[device]).wait()

    q_arrived(at(0, 1))
    attend(chip * 2)
    own_o = pltpu.make_async_copy(mixed.at[me], out.at[:, columns(me)], local_sem.at[3])
    own_o.start()
    send_o(at(0, 1))

    def chip_step(k, carry):
        j = chips - k
        offset = (j + 1) // 2 * (2 * (j % 2) - 1)
        first = at(offset, 0) // 2 * 2
        q_arrived(first)
        q_arrived(first + 1)
        attend(first)
        send_o(first)
        send_o(first + 1)
        return carry

    lax.fori_loop(1, chips, chip_step, 0)

    wait_conv_sends()
    decoded_store.wait()
    own_o.wait()
    arrived(mixed, o_sem, count - 1)
    arrived(v_all, send_sem.at[0], count - 1)
    arrived(k_all, send_sem.at[1], count - 1)
    arrived(q_all, send_sem.at[2], count - 1)
    arrived(mixed, send_sem.at[3], count - 1)


def store_kernel(attended, decoded, attended_out, decoded_out, wide, image, load_sem, store_sem):
    pieces = load_sem.shape[0] - 1
    step = wide.shape[0] // pieces
    moves = [(decoded, image, decoded_out)]
    for i in range(pieces):
        part = pl.ds(i * step, step)
        moves.append((attended.at[part], wide.at[part], attended_out.at[part]))
    loads = [pltpu.make_async_copy(m[0], m[1], load_sem.at[i]) for i, m in enumerate(moves)]
    stores = [pltpu.make_async_copy(m[1], m[2], store_sem.at[i]) for i, m in enumerate(moves)]
    for load in loads:
        load.start()
    for load, store in zip(loads, stores):
        load.wait()
        store.start()
    for store in stores:
        store.wait()


def body(
    queries,
    keys,
    values,
    q_gain,
    k_gain,
    latent_frames,
    frame_cache,
    vae_gain,
    conv_weight,
    conv_bias,
):
    count, roles = lax.axis_size(SEQ), lax.axis_size(ROLE)
    _, rows, width = queries.shape
    depth = HEAD_DIM
    pasts = frame_cache.shape[0]
    _, image_rows, cols, chans = latent_frames.shape
    blocks = (count, rows, depth)
    in_hbm = pl.BlockSpec(memory_space=pltpu.HBM)
    anywhere = pl.BlockSpec(memory_space=pl.ANY)
    low, wide = jnp.bfloat16, jnp.float32
    dma = pltpu.SemaphoreType.DMA
    attended, decoded = pl.pallas_call(
        functools.partial(block_kernel, count, roles),
        out_shape=(
            jax.ShapeDtypeStruct((rows, width), low),
            jax.ShapeDtypeStruct((image_rows, cols, chans), low),
        ),
        in_specs=[in_hbm] * 10,
        out_specs=(anywhere, anywhere),
        scratch_shapes=[
            pltpu.VMEM((rows, width), low),
            pltpu.VMEM((rows, width), low),
            pltpu.VMEM((rows, width), low),
            pltpu.VMEM((1, width), wide),
            pltpu.VMEM((1, width), wide),
            pltpu.VMEM((image_rows, cols, chans), low),
            pltpu.VMEM((pasts, image_rows, cols, chans), low),
            pltpu.VMEM((chans,), wide),
            pltpu.VMEM(conv_weight.shape, low),
            pltpu.VMEM((chans,), wide),
            pltpu.VMEM((3, image_rows + 2, cols, chans), low),
            pltpu.VMEM((pasts, image_rows, cols, chans), low),
            pltpu.VMEM((2, cols * pasts // roles, chans), low),
            pltpu.VMEM((3, image_rows * cols, chans), wide),
            pltpu.VMEM((image_rows, cols, chans), low),
            pltpu.VMEM(blocks, low),
            pltpu.VMEM(blocks, low),
            pltpu.VMEM(blocks, low),
            pltpu.VMEM(blocks, low),
            pltpu.VMEM(blocks, low),
            pltpu.VMEM(blocks, low),
            pltpu.VMEM((2 * rows, rows * count), wide),
            dma((10,)),
            dma((5,)),
            dma((4,)),
            dma,
            dma,
            dma((count,)),
            dma,
            pltpu.SemaphoreType.REGULAR((count // 4 - 1,)),
            dma((2, 2)),
            dma((2, 2)),
            dma((2,)),
            dma((2,)),
            dma((pasts, 2)),
            dma((roles, 2)),
        ],
        compiler_params=pltpu.CompilerParams(
            collective_id=0, has_side_effects=True, vmem_limit_bytes=VMEM_BYTES
        ),
    )(
        queries[0],
        keys[0],
        values[0],
        q_gain.reshape(1, width),
        k_gain.reshape(1, width),
        latent_frames[0],
        frame_cache,
        vae_gain,
        conv_weight,
        conv_bias,
    )
    attended, decoded = pl.pallas_call(
        store_kernel,
        out_shape=(
            jax.ShapeDtypeStruct((rows, width), low),
            jax.ShapeDtypeStruct((image_rows, cols, chans), low),
        ),
        in_specs=[anywhere] * 2,
        out_specs=(anywhere, anywhere),
        scratch_shapes=[
            pltpu.VMEM((rows, width), low),
            pltpu.VMEM((image_rows, cols, chans), low),
            dma((5,)),
            dma((5,)),
        ],
        compiler_params=pltpu.CompilerParams(vmem_limit_bytes=VMEM_BYTES),
    )(attended, decoded)
    return attended[None], decoded[None]


def solution(mesh):
    in_specs = (
        P(("groups", "role"), SEQ, None),
        P(("groups", "role"), SEQ, None),
        P(("groups", "role"), SEQ, None),
        P(),
        P(),
        P(("groups", "role"), SEQ, None, None),
        P("groups", SEQ, None, None),
        P(),
        P(),
        P(),
    )
    out_specs = (P(("groups", "role"), SEQ, None), P(("groups", "role"), SEQ, None, None))
    return jax.shard_map(body, mesh=mesh, in_specs=in_specs, out_specs=out_specs, check_vma=False)
```

```python
import functools

import jax
import jax.numpy as jnp
from jax import lax
from jax.experimental import pallas as pl
from jax.experimental.pallas import tpu as pltpu
from jax.sharding import PartitionSpec as P

HEAD_DIM = 128
SEQ = "seq"
ROLE = "role"
MESH = pl.DeviceIdType.MESH
VMEM_BYTES = 67043328
LOG2_E = 1.4426950408889634


EPSILON = 1e-06


def block_kernel(
    count,
    roles,
    q_in,
    k_in,
    v_in,
    q_gain_in,
    k_gain_in,
    latent_in,
    cache_in,
    vae_gain_in,
    weight_in,
    bias_in,
    out,
    decoded_out,
    q_raw,
    k_raw,
    v_raw,
    q_gain,
    k_gain,
    latent,
    cache,
    vae_gain,
    weight,
    bias,
    frames,
    past,
    past_halo,
    sums,
    decoded,
    q_send,
    k_send,
    q_all,
    k_all,
    v_all,
    mixed,
    scores,
    load_sem,
    local_sem,
    send_sem,
    v_sem,
    k_sem,
    q_sem,
    o_sem,
    wave_sem,
    halo_send,
    halo_sem,
    frame_send,
    frame_sem,
    piece_send,
    piece_sem,
):
    chips = count // 2
    half = chips // 2
    rows, width = q_raw.shape
    depth = width // count
    length = rows * count
    me = lax.axis_index(SEQ)
    chip, core = me // 2, me % 2
    role = lax.axis_index(ROLE)
    image_rows, cols, chans = latent.shape
    pasts = cache.shape[0]
    shares = roles // pasts
    share = cols // shares
    last = image_rows + 1

    def at(offset, other):
        return lax.rem(chip + offset + chips, chips) * 2 + lax.rem(core + other, 2)

    loads = [
        pltpu.make_async_copy(source, target, load_sem.at[i])
        for i, (source, target) in enumerate(
            (
                (v_in, v_raw),
                (latent_in, latent),
                (cache_in, cache),
                (vae_gain_in, vae_gain),
                (k_in, k_raw),
                (k_gain_in, k_gain),
                (q_in, q_raw),
                (q_gain_in, q_gain),
                (weight_in, weight),
                (bias_in, bias),
            )
        )
    ]
    v_load, latent_load, cache_load, vae_gain_load = loads[:4]
    k_load, k_gain_load, q_load, q_gain_load, weight_load, bias_load = loads[4:]
    for load in loads:
        load.start()

    barrier = pltpu.get_barrier_semaphore()
    near = [at(0, 1), at(1, 0), at(1, 1), at(-1, 0), at(-1, 1)]
    for device in near:
        pl.semaphore_signal(barrier, inc=1, device_id={SEQ: device}, device_id_type=MESH)
    for step in range(1, roles):
        pl.semaphore_signal(
            barrier,
            inc=1,
            device_id={ROLE: lax.rem(role + step, roles)},
            device_id_type=MESH,
        )
    pl.semaphore_wait(barrier, len(near) + roles - 1)

    def columns(head):
        return pl.ds(pl.multiple_of(head * depth, depth), depth)

    def to(device, source, target, sem, arrival):
        pltpu.make_async_remote_copy(
            src_ref=source,
            dst_ref=target,
            send_sem=sem,
            recv_sem=arrival,
            device_id={SEQ: device},
            device_id_type=MESH,
        ).start()

    def send_v(device):
        to(device, v_raw.at[:, columns(device)], v_all.at[me], send_sem.at[0], v_sem)

    def send_k(device):
        to(device, k_send.at[device], k_all.at[me], send_sem.at[1], k_sem)

    def send_q(device):
        to(device, q_send.at[device], q_all.at[me], send_sem.at[2], q_sem.at[me])

    v_load.wait()
    own_v = pltpu.make_async_copy(v_raw.at[:, columns(me)], v_all.at[me], local_sem.at[0])
    own_v.start()
    send_v(at(0, 1))

    def activated(values):
        wide = values.astype(jnp.float32)
        mean_sq = jnp.mean(wide * wide, axis=-1, keepdims=True)
        scaled = wide * lax.rsqrt(mean_sq + EPSILON) * vae_gain[...].reshape(1, chans)
        return (scaled * lax.logistic(scaled)).astype(jnp.bfloat16)

    def activate():
        latent_load.wait()
        cache_load.wait()
        vae_gain_load.wait()
        for row in range(image_rows):
            frames[2, 1 + row] = activated(latent[row])
            for frame in range(pasts):
                past[frame, row] = activated(cache[frame, row])

        @pl.when(me == 0)
        def _():
            frames[2, 0] = jnp.zeros((cols, chans), frames.dtype)
            past_halo[0] = jnp.zeros((share, chans), past_halo.dtype)

        @pl.when(me == count - 1)
        def _():
            frames[2, last] = jnp.zeros((cols, chans), frames.dtype)
            past_halo[1] = jnp.zeros((share, chans), past_halo.dtype)

    my_past = role // shares
    my_cols = pl.ds(pl.multiple_of(lax.rem(role, shares) * share, share), share)

    def halo_copies(device, side):
        edge = 0 if side == 0 else image_rows - 1
        landing = 1 - side
        pairs = (
            (frames.at[2, 1 + edge], frames.at[2, landing * last]),
            (past.at[my_past, edge, my_cols], past_halo.at[landing]),
        )
        return [
            pltpu.make_async_remote_copy(
                src_ref=source,
                dst_ref=target,
                send_sem=halo_send.at[side, i],
                recv_sem=halo_sem.at[landing, i],
                device_id={SEQ: device},
                device_id_type=MESH,
            )
            for i, (source, target) in enumerate(pairs)
        ]

    def each_side(act):
        @pl.when(me > 0)
        def _():
            act(me - 1, 0)

        @pl.when(me < count - 1)
        def _():
            act(me + 1, 1)

    def send_halos():
        def start(device, side):
            for copy in halo_copies(device, side):
                copy.start()

        each_side(start)

    def wait_halos():
        def wait(device, side):
            for i, target in enumerate((frames.at[2, side * last], past_halo.at[side])):
                pltpu.make_async_copy(target, target, halo_sem.at[side, i]).wait()

        each_side(wait)

    def frame_copy(ahead):
        return pltpu.make_async_remote_copy(
            src_ref=frames.at[2],
            dst_ref=frames.at[2 - ahead],
            send_sem=frame_send.at[ahead - 1],
            recv_sem=frame_sem.at[ahead - 1],
            device_id={ROLE: role + ahead},
            device_id_type=MESH,
        )

    def piece_place(frame, target, side, source_role):
        part = pl.ds(pl.multiple_of(lax.rem(source_role, shares) * share, share), share)
        return frames.at[frame - target, side * last, part]

    def pieces(act_remote, act_local):
        for target in range(pasts):
            for frame in range(target, pasts):
                for side in range(2):
                    mine = jnp.logical_and(my_past == frame, role != target)
                    here = jnp.logical_and(my_past == frame, role == target)

                    @pl.when(mine)
                    def _():
                        act_remote(frame, target, side)

                    @pl.when(here)
                    def _():
                        act_local(frame, target, side)

    def piece_copy(frame, target, side):
        return pltpu.make_async_remote_copy(
            src_ref=past_halo.at[side],
            dst_ref=piece_place(frame, target, side, role),
            send_sem=piece_send.at[target, side],
            recv_sem=piece_sem.at[role, side],
            device_id={ROLE: target},
            device_id_type=MESH,
        )

    def own_piece(frame, target, side):
        return pltpu.make_async_copy(
            past_halo.at[side],
            piece_place(frame, target, side, role),
            piece_send.at[target, side],
        )

    def pass_on():
        for ahead in (1, 2):

            @pl.when(role + ahead < roles)
            def _():
                frame_copy(ahead).start()

        pieces(
            lambda *which: piece_copy(*which).start(), lambda *which: own_piece(*which).start()
        )
        for target in range(pasts):

            @pl.when(role == target)
            def _():
                for frame in range(target, pasts):
                    frames[frame - target, 1 : 1 + image_rows] = past[frame]

    def wait_frames():
        for ahead in (1, 2):

            @pl.when(role >= ahead)
            def _():
                target = frames.at[2 - ahead]
                pltpu.make_async_copy(target, target, frame_sem.at[ahead - 1]).wait()

        for target in range(pasts):

            @pl.when(role == target)
            def _():
                for source_role in range(target * shares, roles):
                    if source_role == target:
                        continue
                    for side in range(2):
                        place = piece_place(source_role // shares, target, side, source_role)
                        pltpu.make_async_copy(place, place, piece_sem.at[source_role, side]).wait()

        pieces(lambda *which: None, lambda *which: own_piece(*which).wait())

    def wait_conv_sends():
        def wait(device, side):
            for copy in halo_copies(device, side):
                copy.wait_send()

        each_side(wait)
        for ahead in (1, 2):

            @pl.when(role + ahead < roles)
            def _():
                frame_copy(ahead).wait_send()

        pieces(lambda *which: piece_copy(*which).wait_send(), lambda *which: None)

    def convolve():
        flat = image_rows * cols
        sums[...] = jnp.zeros_like(sums)

        def tap(i, carry):
            a, b = i // 3, i % 3
            window = frames[a, pl.ds(b, image_rows)].reshape(flat, chans)
            for e in range(3):
                sums[e] += jnp.dot(window, weight[a, b, e], preferred_element_type=jnp.float32)
            return carry

        lax.fori_loop(0, 9, tap, 0)
        index = lax.broadcasted_iota(jnp.int32, (cols, chans), 0)
        for row in range(image_rows):
            part = pl.ds(row * cols, cols)
            left = jnp.where(index == 0, 0.0, pltpu.roll(sums[0, part], 1, 0))
            right = jnp.where(index == cols - 1, 0.0, pltpu.roll(sums[2, part], cols - 1, 0))
            conv = sums[1, part] + left + right
            decoded[row] = (latent[row].astype(jnp.float32) + conv + bias[...].reshape(1, chans)).astype(
                decoded.dtype
            )

    for d in range(1, half + 1):
        if d > 1:
            for device in near[1:]:
                pl.semaphore_signal(
                    wave_sem.at[d - 2], inc=1, device_id={SEQ: device}, device_id_type=MESH
                )
            pl.semaphore_wait(wave_sem.at[d - 2], len(near) - 1)
        for other in range(2):
            send_v(at(d, other))
            if d < half:
                send_v(at(-d, other))
        if d == 2:
            activate()
            send_halos()

    def normalize(raw, gain, target):
        step = 16

        def some(i, carry):
            at_rows = pl.ds(pl.multiple_of(i * step, step), step)
            wide = raw[at_rows, :].astype(jnp.float32)
            mean_sq = jnp.mean(wide * wide, axis=-1, keepdims=True)
            scaled = (wide * lax.rsqrt(mean_sq + EPSILON) * gain[...]).astype(jnp.bfloat16)
            for head in range(count):
                target[head, at_rows, :] = scaled[:, head * depth : (head + 1) * depth]
            return carry

        lax.fori_loop(0, rows // step, some, 0)

    def send_all(send):
        send(at(0, 1))

        def pair(d, carry):
            for other in range(2):
                send(at(d, other))
                send(at(-d, other))
            return carry

        lax.fori_loop(1, half, pair, 0)
        for other in range(2):
            send(at(half, other))

    k_load.wait()
    k_gain_load.wait()
    normalize(k_raw, k_gain, k_send)
    own_k = pltpu.make_async_copy(k_send.at[me], k_all.at[me], local_sem.at[1])
    own_k.start()
    send_all(send_k)

    q_load.wait()
    q_gain_load.wait()
    normalize(q_raw, q_gain, q_send)
    own_q = pltpu.make_async_copy(q_send.at[me], q_all.at[me], local_sem.at[2])
    own_q.start()

    def farthest_first(i, carry):
        d = half - i
        for other in range(2):
            send_q(at(d, other))
            send_q(at(-d, other))
        return carry

    for other in range(2):
        send_q(at(half, other))
    lax.fori_loop(1, half, farthest_first, 0)
    send_q(at(0, 1))

    wait_halos()
    pass_on()
    weight_load.wait()
    bias_load.wait()
    wait_frames()
    convolve()
    decoded_store = pltpu.make_async_copy(decoded, decoded_out, local_sem.at[4])
    decoded_store.start()

    def arrived(buffer, sem, blocks):
        pltpu.make_async_copy(buffer.at[pl.ds(0, blocks)], buffer.at[pl.ds(0, blocks)], sem).wait()

    own_v.wait()
    own_k.wait()
    own_q.wait()
    arrived(v_all, v_sem, count - 1)
    arrived(k_all, k_sem, count - 1)

    tile = 512
    blocks = tile // rows
    factor = LOG2_E * depth ** (-0.5)
    both = 2 * rows

    def attend(first):
        queries = q_all[pl.ds(first, 2)].reshape(both, depth)
        top = None
        for j in range(length // tile):
            keys = k_all[pl.ds(j * blocks, blocks)].reshape(tile, depth)
            part = lax.dot_general(
                queries, keys, (((1,), (1,)), ((), ())), preferred_element_type=jnp.float32
            )
            scores[:, pl.ds(j * tile, tile)] = part
            for g in range(tile // depth):
                piece = part[:, g * depth : (g + 1) * depth]
                top = piece if top is None else jnp.maximum(top, piece)
        top = jnp.max(top, axis=1, keepdims=True)
        total = jnp.zeros((both, depth), jnp.float32)
        result = jnp.zeros((both, depth), jnp.float32)
        for j in range(length // tile):
            weights = jnp.exp2((scores[:, pl.ds(j * tile, tile)] - top) * factor)
            for g in range(tile // depth):
                total = total + weights[:, g * depth : (g + 1) * depth]
            some_v = v_all[pl.ds(j * blocks, blocks)].reshape(tile, depth)
            result = result + jnp.dot(
                weights.astype(jnp.bfloat16), some_v, preferred_element_type=jnp.float32
            )
        result = result / jnp.sum(total, axis=1, keepdims=True)
        mixed[pl.ds(first, 2)] = result.astype(jnp.bfloat16).reshape(2, rows, depth)

    def send_o(device):
        to(device, mixed.at[device], out.at[:, columns(me)], send_sem.at[3], o_sem)

    def q_arrived(device):
        pltpu.make_async_copy(q_all.at[device], q_all.at[device], q_sem.at[device]).wait()

    def chip_step(k, carry):
        j = chips - k
        offset = (j + 1) // 2 * (2 * (j % 2) - 1)
        first = at(offset, 0) // 2 * 2
        q_arrived(first)
        q_arrived(first + 1)
        attend(first)
        send_o(first)
        send_o(first + 1)
        return carry

    lax.fori_loop(1, chips, chip_step, 0)
    q_arrived(at(0, 1))
    attend(chip * 2)
    own_o = pltpu.make_async_copy(mixed.at[me], out.at[:, columns(me)], local_sem.at[3])
    own_o.start()
    send_o(at(0, 1))

    wait_conv_sends()
    decoded_store.wait()
    own_o.wait()
    arrived(mixed, o_sem, count - 1)
    arrived(v_all, send_sem.at[0], count - 1)
    arrived(k_all, send_sem.at[1], count - 1)
    arrived(q_all, send_sem.at[2], count - 1)
    arrived(mixed, send_sem.at[3], count - 1)


def store_kernel(attended, decoded, attended_out, decoded_out, wide, image, load_sem, store_sem):
    pieces = load_sem.shape[0] - 1
    step = wide.shape[0] // pieces
    moves = [(decoded, image, decoded_out)]
    for i in range(pieces):
        part = pl.ds(i * step, step)
        moves.append((attended.at[part], wide.at[part], attended_out.at[part]))
    loads = [pltpu.make_async_copy(m[0], m[1], load_sem.at[i]) for i, m in enumerate(moves)]
    stores = [pltpu.make_async_copy(m[1], m[2], store_sem.at[i]) for i, m in enumerate(moves)]
    for load in loads:
        load.start()
    for load, store in zip(loads, stores):
        load.wait()
        store.start()
    for store in stores:
        store.wait()


def body(
    queries,
    keys,
    values,
    q_gain,
    k_gain,
    latent_frames,
    frame_cache,
    vae_gain,
    conv_weight,
    conv_bias,
):
    count, roles = lax.axis_size(SEQ), lax.axis_size(ROLE)
    _, rows, width = queries.shape
    depth = HEAD_DIM
    pasts = frame_cache.shape[0]
    _, image_rows, cols, chans = latent_frames.shape
    blocks = (count, rows, depth)
    in_hbm = pl.BlockSpec(memory_space=pltpu.HBM)
    anywhere = pl.BlockSpec(memory_space=pl.ANY)
    low, wide = jnp.bfloat16, jnp.float32
    dma = pltpu.SemaphoreType.DMA
    attended, decoded = pl.pallas_call(
        functools.partial(block_kernel, count, roles),
        out_shape=(
            jax.ShapeDtypeStruct((rows, width), low),
            jax.ShapeDtypeStruct((image_rows, cols, chans), low),
        ),
        in_specs=[in_hbm] * 10,
        out_specs=(anywhere, anywhere),
        scratch_shapes=[
            pltpu.VMEM((rows, width), low),
            pltpu.VMEM((rows, width), low),
            pltpu.VMEM((rows, width), low),
            pltpu.VMEM((1, width), wide),
            pltpu.VMEM((1, width), wide),
            pltpu.VMEM((image_rows, cols, chans), low),
            pltpu.VMEM((pasts, image_rows, cols, chans), low),
            pltpu.VMEM((chans,), wide),
            pltpu.VMEM(conv_weight.shape, low),
            pltpu.VMEM((chans,), wide),
            pltpu.VMEM((3, image_rows + 2, cols, chans), low),
            pltpu.VMEM((pasts, image_rows, cols, chans), low),
            pltpu.VMEM((2, cols * pasts // roles, chans), low),
            pltpu.VMEM((3, image_rows * cols, chans), wide),
            pltpu.VMEM((image_rows, cols, chans), low),
            pltpu.VMEM(blocks, low),
            pltpu.VMEM(blocks, low),
            pltpu.VMEM(blocks, low),
            pltpu.VMEM(blocks, low),
            pltpu.VMEM(blocks, low),
            pltpu.VMEM(blocks, low),
            pltpu.VMEM((2 * rows, rows * count), wide),
            dma((10,)),
            dma((5,)),
            dma((4,)),
            dma,
            dma,
            dma((count,)),
            dma,
            pltpu.SemaphoreType.REGULAR((count // 4 - 1,)),
            dma((2, 2)),
            dma((2, 2)),
            dma((2,)),
            dma((2,)),
            dma((pasts, 2)),
            dma((roles, 2)),
        ],
        compiler_params=pltpu.CompilerParams(
            collective_id=0, has_side_effects=True, vmem_limit_bytes=VMEM_BYTES
        ),
    )(
        queries[0],
        keys[0],
        values[0],
        q_gain.reshape(1, width),
        k_gain.reshape(1, width),
        latent_frames[0],
        frame_cache,
        vae_gain,
        conv_weight,
        conv_bias,
    )
    attended, decoded = pl.pallas_call(
        store_kernel,
        out_shape=(
            jax.ShapeDtypeStruct((rows, width), low),
            jax.ShapeDtypeStruct((image_rows, cols, chans), low),
        ),
        in_specs=[anywhere] * 2,
        out_specs=(anywhere, anywhere),
        scratch_shapes=[
            pltpu.VMEM((rows, width), low),
            pltpu.VMEM((image_rows, cols, chans), low),
            dma((5,)),
            dma((5,)),
        ],
        compiler_params=pltpu.CompilerParams(vmem_limit_bytes=VMEM_BYTES),
    )(attended, decoded)
    return attended[None], decoded[None]


def solution(mesh):
    in_specs = (
        P(("groups", "role"), SEQ, None),
        P(("groups", "role"), SEQ, None),
        P(("groups", "role"), SEQ, None),
        P(),
        P(),
        P(("groups", "role"), SEQ, None, None),
        P("groups", SEQ, None, None),
        P(),
        P(),
        P(),
    )
    out_specs = (P(("groups", "role"), SEQ, None), P(("groups", "role"), SEQ, None, None))
    return jax.shard_map(body, mesh=mesh, in_specs=in_specs, out_specs=out_specs, check_vma=False)
```
